128 devices in a mesh: row: 32 (over z, x, y_lo), col: 4 (over y_hi, core).
Axes of the slice: x: 4, y: 4 (y_hi: 2, y_lo: 2; y = y_hi * 2 + y_lo), z: 4, core: 2. Of those that a mesh axis runs over, the one named last changes fastest.
Arguments:
- trailing: float32 [65536, 8192], P('row', 'col'), may hold values from -6 to 6
- vectors: float32 [65536, 256], P(('row', 'col')), may hold values from -0.09375 to 0.09375
- tfactor: float32 [256, 256], replicated, may hold values from -0.375 to 0.375
Outputs:
- updated: float32 [65536, 8192], P('row', 'col')
The draws below stay inside these ranges and needn't reach their ends.
All inputs are finite; a program needn't handle non-finite values.
Results may differ from the reference program's by a relative error of at most 0.0003.
Values sent between devices are 32-bit elements.
A program may use at most 128 MiB of HBM per device.

```python
import jax
import jax.numpy as jnp
from jax import lax

N = 8192
K = 256
M = 65536


def steps_of(own_key, shape, shards, smallest, high):
    loudness, own = 1.0, jax.random.fold_in(own_key, 6)
    for axis_at, shards_of in shards:
        heights = jnp.exp(jax.random.uniform(jax.random.fold_in(own, axis_at), (shards_of,), jnp.float32, smallest / len(shards), high / len(shards)))
        loudness = loudness * jnp.repeat(heights, shape[axis_at] // shards_of).reshape([-1 if axis == axis_at else 1 for axis in range(len(shape))])
    return loudness


def gaussian(own_key, dims, width, most, split=(), kind=jnp.bfloat16):
    loudness = steps_of(own_key, dims, split, -0.22, 0.18) if split else 1.0
    drawn = jax.random.normal(own_key, dims, jnp.float32) * width * loudness
    return jnp.minimum(jnp.maximum(drawn, -most), most).astype(kind)


def setup_inputs(seed: int = 0) -> dict:
    arg_keys = jax.random.split(jax.random.key(seed), 4)
    return {
        "trailing": gaussian(arg_keys[0], (M, N), 1.0, 6.0, ((0, 32), (1, 4)), jnp.float32),
        "vectors": gaussian(arg_keys[1], (M, K), (M // 16) ** -0.5, 0.09375, ((0, 128),), jnp.float32),
        "tfactor": gaussian(arg_keys[2], (K, K), K ** -0.5, 0.375, (), jnp.float32),
    }


def reference(trailing, vectors, tfactor):
    high = lax.Precision.HIGHEST
    coeffs = jnp.dot(vectors.T, trailing, precision=high, preferred_element_type=jnp.float32)
    scaled = jnp.dot(tfactor, coeffs, precision=high, preferred_element_type=jnp.float32)
    return trailing - jnp.dot(vectors, scaled, precision=high, preferred_element_type=jnp.float32)
```

```python
import functools

import jax
import jax.numpy as jnp
from jax import lax
from jax.experimental import pallas as pl
from jax.experimental.pallas import tpu as pltpu
from jax.sharding import PartitionSpec as P

MESH = pl.DeviceIdType.MESH
F32, BF16 = jnp.float32, jnp.bfloat16

ROWS = 2048
COLS = 2048
K = 256
BLOCK = 512
UNIT = 256
UNITS = COLS // UNIT
PIECES = 4
PIECE = BLOCK // (2 * PIECES)

PLANS = (
    (("xa",), ("za",), ("xb", "zb", "y")),
    (("xb",), ("zb",), ("xa", "za", "y")),
    (("za",), ("xb",), ("xa", "zb", "y")),
    (("zb",), ("xa",), ("xb", "za", "y")),
)
STAGES = 3


def split(value):
    high = value.astype(BF16)
    return high, (value - high.astype(F32)).astype(BF16)


def place():
    row, col = lax.axis_index("row"), lax.axis_index("col")
    z, x, y_low = row // 8, (row // 2) % 4, row % 2
    bits = {
        "xa": (x % 2 + x // 2) % 2,
        "xb": x // 2,
        "za": (z % 2 + z // 2) % 2,
        "zb": z // 2,
        "y": y_low,
    }
    return bits, col


def row_of(bits):
    x = bits["xb"] * 2 + (bits["xa"] + bits["xb"]) % 2
    z = bits["zb"] * 2 + (bits["za"] + bits["zb"]) % 2
    return z * 8 + x * 2 + bits["y"]


def flipped(bits, names):
    return {name: 1 - bit if name in names else bit for name, bit in bits.items()}


def index_of(bits, names):
    index = 0
    for name in names:
        index = index * 2 + bits[name]
    return index


def offsets(names):
    count = len(names)
    return [
        tuple(name for at, name in enumerate(names) if offset >> (count - 1 - at) & 1)
        for offset in range(1, 2**count)
    ]


def gather_reduce(
    c_hbm, v_hbm, t_ref, c_ref, coef, w_ref,
    vall, fwd, vst, part, arrived,
    c_sem, v_sem, s1_send, s1_recv, s2_send, s2_recv, d1_send, d1_recv, d2_send, d2_recv,
    out_send, out_recv,
):
    bits, col = place()
    row = row_of(bits)
    y_high, core = col // 2, col % 2
    y = y_high * 2 + bits["y"]
    sibling = (row, y_high * 2 + 1 - core)
    along = []
    for step in (1, 3):
        there = (y + step) % 4
        base = row - bits["y"]
        along.append((base + there % 2, there // 2 * 2 + core))
    slots = [
        col,
        y_high * 2 + 1 - core,
        (1 - y_high) * 2 + core,
        (1 - y_high) * 2 + 1 - core,
    ]

    v_load = pltpu.make_async_copy(v_hbm, vall.at[slots[0]], v_sem)
    v_load.start()
    c_loads = []
    for at, slot in enumerate(slots):
        rows = pl.ds(pl.multiple_of(slot * BLOCK, BLOCK), BLOCK)
        c_loads.append(pltpu.make_async_copy(c_hbm.at[rows], c_ref.at[rows], c_sem.at[at]))
        c_loads[-1].start()

    met = [(), *{names for plan in PLANS for stage in plan for names in offsets(stage)}]
    met = sorted(met)[1:]
    barrier = pltpu.get_barrier_semaphore()
    greet = [(row_of(flipped(bits, names)), col) for names in met]
    assert ("y",) in met
    other = (y + 1) % 4 * bits["y"] + (y + 3) % 4 * (1 - bits["y"])
    greet += [sibling, (row - bits["y"] + other % 2, other // 2 * 2 + core)]
    for device in greet:
        pl.semaphore_signal(barrier, inc=1, device_id=device, device_id_type=MESH)
    pl.semaphore_wait(barrier, len(greet))

    def remote(src, dst, send, recv, device):
        return pltpu.make_async_remote_copy(
            src_ref=src, dst_ref=dst, send_sem=send, recv_sem=recv,
            device_id=device, device_id_type=MESH,
        )

    sends = []
    v_load.wait()

    def rows_of(direction, piece):
        return pl.ds(piece * 2 * PIECE + direction * PIECE, PIECE)

    first = {}
    for piece in range(PIECES):
        for direction in range(2):
            copy = remote(
                vall.at[slots[0], rows_of(direction, piece)], fwd.at[direction, piece],
                s1_send.at[direction, piece], s1_recv.at[direction, piece], along[direction],
            )
            copy.start()
            first[direction, piece] = copy
        if piece == 0:
            near = remote(vall.at[slots[0]], vall.at[slots[0]], d1_send, d1_recv, sibling)
            near.start()

    def transpose(slot, start, size):
        rows = pl.ds(start, size)
        high, low = split(vall[slot, rows, :].T)
        vst[slot, pl.ds(0, K), rows] = high
        vst[slot, pl.ds(K, K), rows] = low

    def product(unit, slot, start, size):
        columns = pl.ds(pl.multiple_of(unit * UNIT, UNIT), UNIT)
        rows = pl.ds(pl.multiple_of(slot * BLOCK + start, size), size)
        high, low = split(c_ref[rows, columns])
        both = jnp.dot(vst[slot, :, pl.ds(start, size)], high, preferred_element_type=F32)
        return both[:K] + both[K:] + jnp.dot(
            vst[slot, pl.ds(0, K), pl.ds(start, size)], low, preferred_element_type=F32
        )

    transpose(slots[0], 0, BLOCK)
    c_loads[0].wait()

    @pl.loop(0, UNITS)
    def _(unit):
        part[unit] = product(unit, slots[0], 0, BLOCK)

    remote(vall.at[slots[1]], vall.at[slots[1]], d1_send, d1_recv, sibling).wait_recv()
    transpose(slots[1], 0, BLOCK)
    c_loads[1].wait()

    @pl.loop(0, UNITS)
    def _(unit):
        part[unit] += product(unit, slots[1], 0, BLOCK)

    second = {}
    for piece in range(PIECES):
        for direction in range(2):
            first[direction, piece].wait_recv()
            there = (y + (1, 3)[direction]) % 4
            slot = (1 - there // 2) * 2 + core
            copy = remote(
                fwd.at[direction, piece], vall.at[slot, rows_of(direction, piece)],
                s2_send.at[direction, piece], s2_recv.at[direction, piece], along[direction],
            )
            copy.start()
            second[direction, piece] = copy
    third = {}
    for piece in range(PIECES):
        for direction in range(2):
            landed = vall.at[slots[2], rows_of(direction, piece)]
            remote(
                landed, landed, s2_send.at[direction, piece], s2_recv.at[direction, piece],
                along[direction],
            ).wait_recv()
            copy = remote(
                landed, landed, d2_send.at[direction, piece], d2_recv.at[direction, piece], sibling
            )
            copy.start()
            third[direction, piece] = copy
        if piece == PIECES // 2 - 1:
            transpose(slots[2], 0, BLOCK // 2)
            c_loads[2].wait()

            @pl.loop(0, UNITS)
            def _(unit):
                part[unit] += product(unit, slots[2], 0, BLOCK // 2)

    def far(start, stop):
        for piece in range(start, stop):
            for direction in range(2):
                landed = vall.at[slots[3], rows_of(direction, piece)]
                remote(
                    landed, landed, d2_send.at[direction, piece], d2_recv.at[direction, piece],
                    sibling,
                ).wait_recv()

    far(0, PIECES // 2)
    transpose(slots[3], 0, BLOCK // 2)
    c_loads[3].wait()

    @pl.loop(0, UNITS)
    def _(unit):
        part[unit] += product(unit, slots[3], 0, BLOCK // 2)

    transpose(slots[2], BLOCK // 2, BLOCK // 2)
    far(PIECES // 2, PIECES)
    transpose(slots[3], BLOCK // 2, BLOCK // 2)

    bases = [[0] for _ in range(UNITS)]
    spans = []
    size, start = K, 0
    for stage in range(STAGES):
        group = 2 ** len(PLANS[0][stage])
        size //= group
        spans.append((start, size))
        start += (group - 1) * size

    def shard(base, index, size):
        return pl.ds(pl.multiple_of(base + index * size, 8), size)

    def send(unit, stage, gather):
        names = PLANS[unit % 4][stage]
        start, size = spans[stage]
        base = bases[unit][stage]
        mine = index_of(bits, names)
        slot = stage + STAGES if gather else stage
        for at, flip in enumerate(offsets(names)):
            there = flipped(bits, flip)
            if gather:
                src = dst = coef.at[unit, shard(base, mine, size)]
            else:
                src = part.at[unit, shard(base, index_of(there, names), size)]
                dst = arrived.at[unit, pl.ds(start + at * size, size)]
            remote(
                src, dst, out_send.at[unit, slot], out_recv.at[unit, slot], (row_of(there), col)
            ).start()

    def everything(unit, stage, gather):
        names = PLANS[unit % 4][stage]
        start, size = spans[stage]
        slot = stage + STAGES if gather else stage
        whole = arrived.at[unit, pl.ds(start, (2 ** len(names) - 1) * size)]
        return remote(
            whole, whole, out_send.at[unit, slot], out_recv.at[unit, slot],
            (row_of(flipped(bits, names)), col),
        )

    def add(unit, stage):
        names = PLANS[unit % 4][stage]
        start, size = spans[stage]
        mine = shard(bases[unit][stage], index_of(bits, names), size)
        total = part[unit, mine, :]
        for at in range(2 ** len(names) - 1):
            total += arrived[unit, pl.ds(start + at * size, size), :]
        if stage == STAGES - 1:
            coef[unit, mine, :] = total
        else:
            part[unit, mine, :] = total
        bases[unit].append(bases[unit][stage] + index_of(bits, names) * size)

    for unit in range(UNITS):
        part[unit] += product(unit, slots[2], BLOCK // 2, BLOCK // 2) + product(
            unit, slots[3], BLOCK // 2, BLOCK // 2
        )
        send(unit, 0, False)

    t_high, t_low = split(t_ref[...])

    @pl.loop(0, 4)
    def _(slot):
        high, low = split(vall[slot])
        both = jnp.dot(jnp.concatenate([high, low], axis=0), t_high, preferred_element_type=F32)
        product_w = both[:BLOCK] + both[BLOCK:] + jnp.dot(high, t_low, preferred_element_type=F32)
        w_high, w_low = split(product_w)
        w_ref[slot, pl.ds(0, BLOCK), :] = w_high
        w_ref[slot, pl.ds(BLOCK, BLOCK), :] = w_low

    half = UNITS // 2
    for stage in range(STAGES):
        for unit in range(UNITS):
            everything(unit, stage, False).wait_recv()
            add(unit, stage)
            if stage < STAGES - 1:
                send(unit, stage + 1, False)
            else:
                send(unit, stage, True)
    for stage in reversed(range(STAGES)):
        for unit in range(UNITS):
            everything(unit, stage, True).wait_recv()
            if stage:
                send(unit, stage - 1, True)

    near.wait_send()
    for table in (first, second, third):
        for copy in table.values():
            copy.wait_send()
    for unit in range(UNITS):
        for stage in range(STAGES):
            for gather in (False, True):
                everything(unit, stage, gather).wait_send()


TILES = 4
TILE = ROWS // TILES


def update(c_ref, coef, w_ref, out_hbm, chl, obuf, sem):
    @pl.loop(0, UNITS)
    def _(unit):
        high, low = split(coef[unit])
        chl[0, unit] = high
        chl[1, unit] = low

    copies = []
    for tile in range(TILES):
        rows = pl.ds(tile * TILE, TILE)
        if tile >= 2:
            copies[tile - 2].wait()

        @pl.loop(0, UNITS)
        def _(unit):
            columns = pl.ds(pl.multiple_of(unit * UNIT, UNIT), UNIT)
            both = jnp.dot(w_ref[tile], chl[0, unit], preferred_element_type=F32)
            change = both[:TILE] + both[TILE:] + jnp.dot(
                w_ref[tile, pl.ds(0, TILE), :], chl[1, unit], preferred_element_type=F32
            )
            obuf[tile % 2, :, columns] = c_ref[rows, columns] - change

        copy = pltpu.make_async_copy(obuf.at[tile % 2], out_hbm.at[rows], sem.at[tile % 2])
        copy.start()
        copies.append(copy)
    for copy in copies[-2:]:
        copy.wait()


def shards(trailing, vectors, tfactor):
    anywhere = pl.BlockSpec(memory_space=pl.ANY)
    vmem = pl.BlockSpec(memory_space=pltpu.VMEM)
    dma = pltpu.SemaphoreType.DMA
    c, coef, w = pl.pallas_call(
        gather_reduce,
        out_shape=(
            pltpu.VMEM((ROWS, COLS), F32),
            pltpu.VMEM((UNITS, K, UNIT), F32),
            pltpu.VMEM((4, 2 * BLOCK, K), BF16),
        ),
        in_specs=[anywhere, anywhere, vmem],
        out_specs=(vmem, vmem, vmem),
        scratch_shapes=[
            pltpu.VMEM((4, BLOCK, K), F32),
            pltpu.VMEM((2, PIECES, PIECE, K), F32),
            pltpu.VMEM((4, 2 * K, BLOCK), BF16),
            pltpu.VMEM((UNITS, K, UNIT), F32),
            pltpu.VMEM((UNITS, 248, UNIT), F32),
            dma((4,)), dma(()),
            dma((2, PIECES)), dma((2, PIECES)), dma((2, PIECES)), dma((2, PIECES)),
            dma(()), dma(()), dma((2, PIECES)), dma((2, PIECES)),
            dma((UNITS, 2 * STAGES)), dma((UNITS, 2 * STAGES)),
        ],
        compiler_params=pltpu.CompilerParams(
            collective_id=0, has_side_effects=True, vmem_limit_bytes=24 * 2**20
        ),
        cost_estimate=pl.CostEstimate(flops=2 * ROWS * COLS * K, bytes_accessed=2**24, transcendentals=0),
        name="gather_reduce",
    )(trailing, vectors, tfactor)
    return pl.pallas_call(
        update,
        out_shape=jax.ShapeDtypeStruct((ROWS, COLS), F32),
        in_specs=[vmem, vmem, vmem],
        out_specs=anywhere,
        scratch_shapes=[
            pltpu.VMEM((2, UNITS, K, UNIT), BF16),
            pltpu.VMEM((2, TILE, COLS), F32),
            dma((2,)),
        ],
        compiler_params=pltpu.CompilerParams(vmem_limit_bytes=20 * 2**20),
        cost_estimate=pl.CostEstimate(flops=2 * ROWS * COLS * K, bytes_accessed=2**24, transcendentals=0),
        name="update",
    )(c, coef, w)


def solution(mesh):
    placed = (P("row", "col"), P(("row", "col"), None), P())
    return jax.shard_map(
        shards, mesh=mesh, in_specs=placed, out_specs=P("row", "col"), check_vma=False
    )
```

```python
import jax
import jax.numpy as jnp
from jax import lax
from jax.experimental import pallas as pl
from jax.experimental.pallas import tpu as pltpu
from jax.sharding import PartitionSpec as P

MESH = pl.DeviceIdType.MESH
F32, BF16 = jnp.float32, jnp.bfloat16

ROWS = 2048
COLS = 2048
K = 256
HALF = K // 2
BLOCK = 512
WIDE = COLS // 4
UNITS = 8
PIECES = 2
PIECE = BLOCK // (2 * PIECES)

PLANS = (
    (("xa",), ("za",), ("xb", "zb", "y")),
    (("xb",), ("zb",), ("xa", "za", "y")),
    (("za",), ("xb",), ("xa", "zb", "y")),
    (("zb",), ("xa",), ("xb", "za", "y")),
)
STAGES = 3


def split(value):
    high = value.astype(BF16)
    return high, (value - high.astype(F32)).astype(BF16)


def dot(left, right):
    return jnp.dot(left, right, preferred_element_type=F32)


def place():
    row, col = lax.axis_index("row"), lax.axis_index("col")
    z, x, y_low = row // 8, (row // 2) % 4, row % 2
    bits = {
        "xa": (x % 2 + x // 2) % 2,
        "xb": x // 2,
        "za": (z % 2 + z // 2) % 2,
        "zb": z // 2,
        "y": y_low,
    }
    return bits, col


def row_of(bits):
    x = bits["xb"] * 2 + (bits["xa"] + bits["xb"]) % 2
    z = bits["zb"] * 2 + (bits["za"] + bits["zb"]) % 2
    return z * 8 + x * 2 + bits["y"]


def flipped(bits, names):
    return {name: 1 - bit if name in names else bit for name, bit in bits.items()}


def index_of(bits, names):
    index = 0
    for name in names:
        index = index * 2 + bits[name]
    return index


def offsets(names):
    count = len(names)
    return [
        tuple(name for at, name in enumerate(names) if offset >> (count - 1 - at) & 1)
        for offset in range(1, 2**count)
    ]


def gather_reduce(
    c_hbm, v_hbm, t_hbm, c_ref, rhs, w_ref,
    t_ref, vall, fwd, vst, part, coef, arrived_0, arrived_1, arrived_2,
    c_sem, v_sem, t_sem,
    s1_send, s1_recv, s2_send, s2_recv, d1_send, d1_recv, d2_send, d2_recv,
    out_send, out_recv,
):
    bits, col = place()
    row = row_of(bits)
    y_high, core = col // 2, col % 2
    y = y_high * 2 + bits["y"]
    sibling = (row, y_high * 2 + 1 - core)
    along = []
    for step in (1, 3):
        there = (y + step) % 4
        along.append((row - bits["y"] + there % 2, there // 2 * 2 + core))
    slots = [
        col,
        y_high * 2 + 1 - core,
        (1 - y_high) * 2 + core,
        (1 - y_high) * 2 + 1 - core,
    ]

    v_loads = []
    for half in range(2):
        v_loads.append(pltpu.make_async_copy(
            v_hbm.at[:, pl.ds(half * HALF, HALF)], vall.at[slots[0], half], v_sem.at[half]
        ))
        v_loads[-1].start()
    t_load = pltpu.make_async_copy(t_hbm, t_ref, t_sem)
    t_load.start()
    c_loads = []
    for at, slot in enumerate(slots):
        rows = pl.ds(pl.multiple_of(slot * BLOCK, BLOCK), BLOCK)
        c_loads.append(pltpu.make_async_copy(c_hbm.at[rows], c_ref.at[rows], c_sem.at[at]))
        c_loads[-1].start()

    barrier = pltpu.get_barrier_semaphore()
    met = sorted({names for plan in PLANS for stage in plan for names in offsets(stage)})
    greet = [(row_of(flipped(bits, names)), col) for names in met]
    other = (y + 1) % 4 * bits["y"] + (y + 3) % 4 * (1 - bits["y"])
    greet += [sibling, (row - bits["y"] + other % 2, other // 2 * 2 + core)]
    for device in greet:
        pl.semaphore_signal(barrier, inc=1, device_id=device, device_id_type=MESH)
    pl.semaphore_wait(barrier, len(greet))

    def remote(src, dst, send, recv, device):
        return pltpu.make_async_remote_copy(
            src_ref=src, dst_ref=dst, send_sem=send, recv_sem=recv,
            device_id=device, device_id_type=MESH,
        )

    def rows_of(direction, piece):
        return pl.ds(direction * (BLOCK // 2) + piece * PIECE, PIECE)

    order = [(half, piece, way) for half in range(2) for piece in range(PIECES) for way in range(2)]
    first, second, third, near = {}, {}, {}, []
    for half, piece, way in order:
        key = half, way, piece
        if not (piece or way):
            v_loads[half].wait()
        first[key] = remote(
            vall.at[slots[0], half, rows_of(way, piece)], fwd.at[key],
            s1_send.at[key], s1_recv.at[key], along[way],
        )
        first[key].start()
        if piece == PIECES - 1 and way:
            own = vall.at[slots[0], half]
            near.append(remote(own, own, d1_send.at[half], d1_recv.at[half], sibling))
            near[-1].start()

    def transpose(slot, half):
        high, low = split(vall[slot, half].T)
        vst[slot, pl.ds(half * K, HALF), :] = high
        vst[slot, pl.ds(half * K + HALF, HALF), :] = low

    def block_of(slot, columns):
        return split(c_ref[pl.ds(pl.multiple_of(slot * BLOCK, BLOCK), BLOCK), columns])

    def whole_product(slot, fresh):
        @pl.loop(0, 2)
        def _(side):
            high, low = block_of(slot, pl.ds(pl.multiple_of(side * 2 * WIDE, 2 * WIDE), 2 * WIDE))
            both = dot(vst[slot], high)
            rest = dot(jnp.concatenate([vst[slot, :HALF], vst[slot, K : K + HALF]], axis=0), low)
            for half in range(2):
                at = half * K
                total = (
                    both[at : at + HALF] + both[at + HALF : at + K]
                    + rest[half * HALF : (half + 1) * HALF]
                )
                for place_in in range(2):
                    unit = half * 4 + side * 2 + place_in
                    value = total[:, place_in * WIDE : (place_in + 1) * WIDE]
                    if fresh:
                        part[unit] = value
                    else:
                        part[unit] += value

    def half_product(half, color):
        columns = pl.ds(color * WIDE, WIDE)
        total = part[half * 4 + color]
        for slot in slots[2:]:
            high, low = block_of(slot, columns)
            both = dot(vst[slot, pl.ds(half * K, K), :], high)
            total += both[:HALF] + both[HALF:] + dot(vst[slot, pl.ds(half * K, HALF), :], low)
        part[half * 4 + color] = total

    for half in range(2):
        transpose(slots[0], half)
    c_loads[0].wait()
    whole_product(slots[0], True)
    for half in range(2):
        landed = vall.at[slots[1], half]
        remote(landed, landed, d1_send.at[half], d1_recv.at[half], sibling).wait_recv()
        transpose(slots[1], half)
    c_loads[1].wait()
    whole_product(slots[1], False)

    for half, piece, way in order:
        key = half, way, piece
        first[key].wait_recv()
        there = (y + (1, 3)[way]) % 4
        slot = (1 - there // 2) * 2 + core
        second[key] = remote(
            fwd.at[key], vall.at[slot, half, rows_of(way, piece)],
            s2_send.at[key], s2_recv.at[key], along[way],
        )
        second[key].start()

    def share(half, piece):
        for way in range(2):
            key = half, way, piece
            landed = vall.at[slots[2], half, rows_of(way, piece)]
            remote(landed, landed, s2_send.at[key], s2_recv.at[key], along[way]).wait_recv()
            third[key] = remote(landed, landed, d2_send.at[key], d2_recv.at[key], sibling)
            third[key].start()

    def shared(half):
        for piece in range(PIECES):
            for way in range(2):
                key = half, way, piece
                landed = vall.at[slots[3], half, rows_of(way, piece)]
                remote(landed, landed, d2_send.at[key], d2_recv.at[key], sibling).wait_recv()

    arrived = (arrived_0, arrived_1, arrived_2)
    bases = [[0] for _ in range(UNITS)]
    sizes = [HALF // 2, HALF // 4, HALF // 16]

    def shard(unit, stage, index):
        base = bases[unit][stage]
        if stage < STAGES - 1:
            return pl.ds(pl.multiple_of(base + index * sizes[stage], 8), sizes[stage]), pl.ds(0, WIDE)
        columns = pl.ds(pl.multiple_of(index % 2 * (WIDE // 2), WIDE // 2), WIDE // 2)
        return pl.ds(pl.multiple_of(base + index // 2 * 8, 8), 8), columns

    def send(unit, stage, gather):
        names = PLANS[unit % 4][stage]
        mine = index_of(bits, names)
        slot = stage + STAGES if gather else stage
        for at, flip in enumerate(offsets(names)):
            there = flipped(bits, flip)
            if gather:
                src = dst = coef.at[(unit, *shard(unit, stage, mine))]
            else:
                src = part.at[(unit, *shard(unit, stage, index_of(there, names)))]
                dst = arrived[stage].at[unit, at]
            remote(
                src, dst, out_send.at[unit, slot], out_recv.at[unit, slot], (row_of(there), col)
            ).start()

    def everything(unit, stage, gather):
        names = PLANS[unit % 4][stage]
        slot = stage + STAGES if gather else stage
        whole = arrived[stage].at[unit]
        return remote(
            whole, whole, out_send.at[unit, slot], out_recv.at[unit, slot],
            (row_of(flipped(bits, names)), col),
        )

    def add(unit, stage):
        names = PLANS[unit % 4][stage]
        index = index_of(bits, names)
        mine = (unit, *shard(unit, stage, index))
        total = part[mine]
        for at in range(2 ** len(names) - 1):
            total += arrived[stage][unit, at]
        if stage == STAGES - 1:
            coef[mine] = total
        else:
            part[mine] = total
        bases[unit].append(bases[unit][stage] + index * sizes[stage])

    for piece in range(PIECES):
        share(0, piece)
    transpose(slots[2], 0)
    shared(0)
    transpose(slots[3], 0)
    c_loads[2].wait()
    c_loads[3].wait()
    for color in range(4):
        half_product(0, color)
        send(color, 0, False)
        if color % 2:
            share(1, color // 2)
    transpose(slots[2], 1)
    shared(1)
    transpose(slots[3], 1)
    for color in range(4):
        half_product(1, color)
        send(4 + color, 0, False)

    t_load.wait()
    t_high, t_low = split(t_ref[...])

    @pl.loop(0, 4)
    def _(slot):
        high, low = split(jnp.concatenate([vall[slot, 0], vall[slot, 1]], axis=1))
        both = dot(jnp.concatenate([high, low], axis=0), t_high)
        w_high, w_low = split(both[:BLOCK] + both[BLOCK:] + dot(high, t_low))
        rows = pl.ds(pl.multiple_of(slot * BLOCK, BLOCK), BLOCK)
        w_ref[rows, pl.ds(0, K)] = w_high
        w_ref[rows, pl.ds(K, K)] = w_low
        w_ref[rows, pl.ds(2 * K, K)] = w_high

    for stage in range(STAGES):
        for unit in range(UNITS):
            everything(unit, stage, False).wait_recv()
            add(unit, stage)
            if stage < STAGES - 1:
                send(unit, stage + 1, False)
            else:
                send(unit, stage, True)
    for stage in reversed(range(STAGES)):
        for unit in range(UNITS):
            everything(unit, stage, True).wait_recv()
            if stage:
                send(unit, stage - 1, True)
            else:
                high, low = split(coef[unit])
                columns = pl.ds(unit % 4 * WIDE, WIDE)
                for at, value in ((0, high), (K, high), (2 * K, low)):
                    rhs[pl.ds(at + unit // 4 * HALF, HALF), columns] = value

    for table in (first, second, third):
        for copy in table.values():
            copy.wait_send()
    for copy in near:
        copy.wait_send()
    for unit in range(UNITS):
        for stage in range(STAGES):
            for gather in (False, True):
                everything(unit, stage, gather).wait_send()


TILES = 4
TILE = ROWS // TILES


def update(c_ref, rhs, w_ref, out_hbm, obuf, sem):
    def write(tile):
        rows = pl.ds(pl.multiple_of(tile * TILE, TILE), TILE)
        return pltpu.make_async_copy(obuf.at[tile % 2], out_hbm.at[rows], sem.at[tile % 2])

    @pl.loop(0, TILES)
    def _(tile):
        @pl.when(tile >= 2)
        def _():
            write(tile - 2).wait()

        rows = pl.ds(pl.multiple_of(tile * TILE, TILE), TILE)
        obuf[tile % 2] = c_ref[rows, :] - dot(w_ref[rows, :], rhs[...])
        write(tile).start()

    write(TILES - 2).wait()
    write(TILES - 1).wait()


def shards(trailing, vectors, tfactor):
    hbm = pl.BlockSpec(memory_space=pltpu.HBM)
    vmem = pl.BlockSpec(memory_space=pltpu.VMEM)
    dma = pltpu.SemaphoreType.DMA
    pieces = dma((2, 2, PIECES))
    cost = pl.CostEstimate(flops=2 * ROWS * COLS * K, bytes_accessed=2**24, transcendentals=0)
    c, rhs, w = pl.pallas_call(
        gather_reduce,
        out_shape=(
            pltpu.VMEM((ROWS, COLS), F32),
            pltpu.VMEM((3 * K, COLS), BF16),
            pltpu.VMEM((ROWS, 3 * K), BF16),
        ),
        in_specs=[hbm, hbm, hbm],
        out_specs=(vmem, vmem, vmem),
        scratch_shapes=[
            pltpu.VMEM((K, K), F32),
            pltpu.VMEM((4, 2, BLOCK, HALF), F32),
            pltpu.VMEM((2, 2, PIECES, PIECE, HALF), F32),
            pltpu.VMEM((4, 2 * K, BLOCK), BF16),
            pltpu.VMEM((UNITS, HALF, WIDE), F32),
            pltpu.VMEM((UNITS, HALF, WIDE), F32),
            pltpu.VMEM((UNITS, 1, HALF // 2, WIDE), F32),
            pltpu.VMEM((UNITS, 1, HALF // 4, WIDE), F32),
            pltpu.VMEM((UNITS, 7, 8, WIDE // 2), F32),
            dma((4,)), dma((2,)), dma(()),
            pieces, pieces, pieces, pieces,
            dma((2,)), dma((2,)), pieces, pieces,
            dma((UNITS, 2 * STAGES)), dma((UNITS, 2 * STAGES)),
        ],
        compiler_params=pltpu.CompilerParams(
            collective_id=0, has_side_effects=True, vmem_limit_bytes=24 * 2**20
        ),
        cost_estimate=cost,
        name="gather_reduce",
    )(*(pltpu.with_memory_space_constraint(each, pltpu.HBM) for each in (trailing, vectors, tfactor)))
    return pl.pallas_call(
        update,
        out_shape=jax.ShapeDtypeStruct((ROWS, COLS), F32),
        in_specs=[vmem, vmem, vmem],
        out_specs=hbm,
        scratch_shapes=[pltpu.VMEM((2, TILE, COLS), F32), dma((2,))],
        compiler_params=pltpu.CompilerParams(vmem_limit_bytes=20 * 2**20),
        cost_estimate=cost,
        name="update",
    )(c, rhs, w)


def solution(mesh):
    placed = (P("row", "col"), P(("row", "col"), None), P())
    return jax.shard_map(
        shards, mesh=mesh, in_specs=placed, out_specs=P("row", "col"), check_vma=False
    )
```

```python
import jax
import jax.numpy as jnp
from jax import lax
from jax.experimental import pallas as pl
from jax.experimental.pallas import tpu as pltpu
from jax.sharding import PartitionSpec as P

MESH = pl.DeviceIdType.MESH
F32, BF16 = jnp.float32, jnp.bfloat16

ROWS = 2048
COLS = 2048
K = 256
HALF = K // 2
PARTS = 4
PART = K // PARTS
BLOCK = 512
COLORS = 4
SUBS = 2
WIDE = COLS // (COLORS * SUBS)
UNITS = 2 * SUBS * COLORS

PLANS = (
    (("zb",), ("xa",), ("xb", "y", "za")),
    (("xa",), ("zb",), ("xb", "y", "za")),
    (("za",), ("xb",), ("xa", "zb", "y")),
    (("xb",), ("za",), ("xa", "y", "zb")),
    (("y", "zb"), ("xa",), ("xb", "za")),
    (("xb",), ("y", "zb"), ("xa", "za")),
    (("y",), ("xb", "za"), ("xa", "zb")),
    (("zb",), ("xa",), ("xb", "y", "za")),
    (("xa",), ("y", "zb"), ("xb", "za")),
    (("y",), ("xb", "za"), ("xa", "zb")),
    (("za",), ("xa",), ("xb", "y", "zb")),
    (("xa",), ("y", "za"), ("xb", "zb")),
    (("za",), ("xa",), ("xb", "y", "zb")),
    (("xb",), ("zb",), ("xa", "za", "y")),
    (("y",), ("xb", "za"), ("xa", "zb")),
    (("zb",), ("xa",), ("xb", "y", "za")),
)
ORDER = (
    (0, 0), (1, 0), (2, 0), (3, 0), (4, 0), (5, 0), (6, 0), (7, 0),
    (8, 0), (9, 0), (10, 0), (11, 0), (12, 0), (13, 0), (14, 0), (15, 0),
    (-1, 0), (0, 1), (1, 1), (2, 1), (3, 1), (4, 1), (5, 1), (6, 1),
    (7, 1), (8, 1), (9, 1), (10, 1), (11, 1), (12, 1), (13, 1), (14, 1),
    (15, 1), (-1, 1), (0, 2), (1, 2), (2, 2), (3, 2), (4, 2), (5, 2),
    (6, 2), (7, 2), (8, 2), (9, 2), (10, 2), (11, 2), (12, 2), (13, 2),
    (14, 2), (15, 2), (-1, 2), (-1, 3), (0, 3), (1, 3), (2, 3), (3, 3),
    (4, 3), (5, 3), (6, 3), (7, 3), (8, 3), (9, 3), (10, 3), (11, 3),
    (0, 4), (1, 4), (2, 4), (3, 4), (12, 3), (13, 3), (14, 3), (15, 3),
    (4, 4), (5, 4), (6, 4), (7, 4), (8, 4), (9, 4), (10, 4), (11, 4),
    (0, 5), (1, 5), (2, 5), (3, 5), (12, 4), (13, 4), (14, 4), (15, 4),
    (4, 5), (5, 5), (6, 5), (7, 5), (8, 5), (9, 5), (10, 5), (11, 5),
    (12, 5), (13, 5), (14, 5), (15, 5),
)
MOST = max(len(plan) for plan in PLANS)


def split(value):
    high = value.astype(BF16)
    return high, (value - high.astype(F32)).astype(BF16)


def dot(left, right):
    return jnp.dot(left, right, preferred_element_type=F32)


def place():
    row, col = lax.axis_index("row"), lax.axis_index("col")
    z, x, y_low = row // 8, (row // 2) % 4, row % 2
    bits = {
        "xa": (x % 2 + x // 2) % 2,
        "xb": x // 2,
        "za": (z % 2 + z // 2) % 2,
        "zb": z // 2,
        "y": y_low,
    }
    return bits, col


def row_of(bits):
    x = bits["xb"] * 2 + (bits["xa"] + bits["xb"]) % 2
    z = bits["zb"] * 2 + (bits["za"] + bits["zb"]) % 2
    return z * 8 + x * 2 + bits["y"]


def flipped(bits, names):
    return {name: 1 - bit if name in names else bit for name, bit in bits.items()}


def index_of(bits, names):
    index = 0
    for name in names:
        index = index * 2 + bits[name]
    return index


def offsets(names):
    count = len(names)
    return [
        tuple(name for at, name in enumerate(names) if offset >> (count - 1 - at) & 1)
        for offset in range(1, 2**count)
    ]


def gather_reduce(
    c_hbm, v_hbm, t_hbm, c_ref, rhs, w_ref,
    v_ref, t_ref, vt, fwd, vst, vfar, c_high, c_low, part, coef, arrived,
    c_sem, v_sem, t_sem,
    s1_send, s1_recv, s2_send, s2_recv, d1_send, d1_recv, d2_send, d2_recv,
    out_send, out_recv,
):
    bits, col = place()
    row = row_of(bits)
    y_high, core = col // 2, col % 2
    y = y_high * 2 + bits["y"]
    sibling = (row, y_high * 2 + 1 - core)
    along = []
    for step in (1, 3):
        there = (y + step) % 4
        along.append((row - bits["y"] + there % 2, there // 2 * 2 + core))
    slots = [
        col,
        y_high * 2 + 1 - core,
        (1 - y_high) * 2 + core,
        (1 - y_high) * 2 + 1 - core,
    ]

    v_load = pltpu.make_async_copy(v_hbm, v_ref, v_sem)
    t_load = pltpu.make_async_copy(t_hbm, t_ref, t_sem)
    c_loads = []
    for at, slot in enumerate(slots):
        rows = pl.ds(pl.multiple_of(slot * BLOCK, BLOCK), BLOCK)
        c_loads.append(pltpu.make_async_copy(c_hbm.at[rows], c_ref.at[rows], c_sem.at[at]))
    v_load.start()
    c_loads[0].start()

    barrier = pltpu.get_barrier_semaphore()
    met = {frozenset(names) for plan in PLANS for stage in plan for names in offsets(stage)} | {frozenset(("y",))}
    met = sorted(sorted(names) for names in met)
    greet = [(row_of(flipped(bits, names)), col) for names in met]
    other = (y + 1) % 4 * bits["y"] + (y + 3) % 4 * (1 - bits["y"])
    greet += [sibling, (row - bits["y"] + other % 2, other // 2 * 2 + core)]
    for device in greet:
        pl.semaphore_signal(barrier, inc=1, device_id=device, device_id_type=MESH)

    v_load.wait()
    c_loads[1].start()
    t_load.start()
    vt[slots[0]] = v_ref[...].T
    pl.semaphore_wait(barrier, len(greet))

    def remote(src, dst, send, recv, device):
        return pltpu.make_async_remote_copy(
            src_ref=src, dst_ref=dst, send_sem=send, recv_sem=recv,
            device_id=device, device_id_type=MESH,
        )

    def piece(slot, q, way):
        return vt.at[slot, pl.ds(q * PART, PART), pl.ds(way * (BLOCK // 2), BLOCK // 2)]

    order = [(q, way) for q in range(PARTS) for way in range(2)]
    for q, way in order:
        remote(
            piece(slots[0], q, way), fwd.at[q, way], s1_send, s1_recv.at[q], along[way]
        ).start()
    near = remote(vt.at[slots[0]], vt.at[slots[0]], d1_send, d1_recv, sibling)
    near.start()

    def halves(slot):
        high, low = split(vt[slot])
        vst[slot, pl.ds(0, K), :] = high
        vst[slot, pl.ds(K, K), :] = low

    def unit_of(half, column):
        return half * SUBS * COLORS + column % SUBS * COLORS + column // SUBS

    def whole_product(slot, fresh):
        @pl.loop(0, 2)
        def _(side):
            rows = pl.ds(pl.multiple_of(slot * BLOCK, BLOCK), BLOCK)
            columns = pl.ds(pl.multiple_of(side * 4 * WIDE, 4 * WIDE), 4 * WIDE)
            high, low = split(c_ref[rows, columns])
            both = dot(vst[slot], high)
            total = both[:K] + both[K:] + dot(vst[slot, :K], low)
            for half in range(2):
                for column in range(4):
                    unit = unit_of(half, side * 4 + column)
                    value = total[half * HALF : (half + 1) * HALF, column * WIDE : (column + 1) * WIDE]
                    if fresh:
                        part[unit] = value
                    else:
                        part[unit] += value

    halves(slots[0])
    c_loads[0].wait()
    c_loads[2].start()
    c_loads[3].start()
    whole_product(slots[0], True)
    remote(vt.at[slots[1]], vt.at[slots[1]], d1_send, d1_recv, sibling).wait_recv()
    halves(slots[1])
    c_loads[1].wait()
    whole_product(slots[1], False)

    for q in range(PARTS):
        remote(fwd.at[q], fwd.at[q], s1_send, s1_recv.at[q], along[0]).wait_recv()
        for way in range(2):
            there = (y + (1, 3)[way]) % 4
            remote(
                fwd.at[q, way], piece((1 - there // 2) * 2 + core, q, way),
                s2_send, s2_recv.at[q], along[way],
            ).start()
        if q % 2 == 0:
            c_loads[2 + q // 2].wait()

        @pl.loop(0, 4)
        def _(step):
            size = BLOCK // 8
            start = q % 2 * (BLOCK // 2) + step * size
            rows = pl.ds(pl.multiple_of(slots[2 + q // 2] * BLOCK + start, size), size)
            high, low = split(c_ref[rows, :])
            into = pl.ds(pl.multiple_of(q // 2 * BLOCK + start, size), size)
            c_high[into, :] = high
            c_low[into, :] = low

    def quarter(slot, q):
        return vt.at[slot, pl.ds(q * PART, PART)]

    def share(q):
        landed = quarter(slots[2], q)
        remote(landed, landed, s2_send, s2_recv.at[q], along[0]).wait_recv()
        remote(landed, landed, d2_send, d2_recv.at[q], sibling).start()

    def shared(q):
        landed = quarter(slots[3], q)
        remote(landed, landed, d2_send, d2_recv.at[q], sibling).wait_recv()

    def far_halves(at, half):
        high, low = split(vt[slots[2 + at], pl.ds(half * HALF, HALF), :])
        vfar[half, at, pl.ds(0, HALF), :] = high
        vfar[half, at, pl.ds(HALF, HALF), :] = low

    def far_product(at, half, start, count):
        rows, columns = pl.ds(at * BLOCK, BLOCK), pl.ds(start * WIDE, count * WIDE)
        both = dot(vfar[half, at], c_high[rows, columns])
        total = both[:HALF] + both[HALF:] + dot(
            vfar[half, at, pl.ds(0, HALF), :], c_low[rows, columns]
        )
        for column in range(count):
            part[unit_of(half, start + column)] += total[:, column * WIDE : (column + 1) * WIDE]

    bases = [[0] for _ in range(UNITS)]

    def shape_of(unit, stage):
        start, bits_so_far = 0, 0
        for names in PLANS[unit][: stage + 1]:
            last = start
            bits_so_far += len(names)
            rows = max(HALF >> bits_so_far, 8)
            start += (2 ** len(names) - 1) * rows
        return rows, WIDE if bits_so_far < 5 else WIDE // 2, last

    def shard(unit, stage, index):
        rows, columns, _ = shape_of(unit, stage)
        base = bases[unit][stage]
        if columns == WIDE:
            return pl.ds(pl.multiple_of(base + index * rows, 8), rows), pl.ds(0, WIDE)
        at = pl.ds(pl.multiple_of(index % 2 * columns, columns), columns)
        return pl.ds(pl.multiple_of(base + index // 2 * rows, 8), rows), at

    def arrival(unit, stage, at, count):
        rows, columns, start = shape_of(unit, stage)
        return arrived.at[unit, pl.ds(start + at * rows, count * rows), pl.ds(0, columns)]

    def steps_of(unit):
        return 2 * len(PLANS[unit])

    def send(unit, step):
        gather = step >= len(PLANS[unit])
        stage = steps_of(unit) - 1 - step if gather else step
        names = PLANS[unit][stage]
        for at, flip in enumerate(offsets(names)):
            there = flipped(bits, flip)
            if gather:
                src = dst = coef.at[(unit, *shard(unit, stage, index_of(bits, names)))]
            else:
                src = part.at[(unit, *shard(unit, stage, index_of(there, names)))]
                dst = arrival(unit, stage, at, 1)
            remote(
                src, dst, out_send.at[int(gather)], out_recv.at[unit, step], (row_of(there), col)
            ).start()

    def wait_step(unit, step):
        stage = min(step, steps_of(unit) - 1 - step)
        whole = arrival(unit, stage, 0, 2 ** len(PLANS[unit][stage]) - 1)
        remote(whole, whole, out_send.at[0], out_recv.at[unit, step], sibling).wait_recv()

    def add(unit, stage):
        names = PLANS[unit][stage]
        index = index_of(bits, names)
        mine = (unit, *shard(unit, stage, index))
        rows, columns, start = shape_of(unit, stage)
        total = part[mine]
        for at in range(2 ** len(names) - 1):
            total += arrived[unit, pl.ds(start + at * rows, rows), pl.ds(0, columns)]
        if stage == len(PLANS[unit]) - 1:
            coef[mine] = total
        else:
            part[mine] = total
        bases[unit].append(bases[unit][stage] + index * rows)

    share(0)
    for half in range(2):
        share(2 * half + 1)
        far_halves(0, half)
        far_product(0, half, 0, 4)
        far_product(0, half, 4, 4)
        shared(2 * half)
        shared(2 * half + 1)
        far_halves(1, half)
        for color in range(COLORS):
            far_product(1, half, color * SUBS, SUBS)
            for sub in range(SUBS):
                send(unit_of(half, color * SUBS + sub), 0)
            if half == 0 and color == 1:
                share(2)

    def weights(slot):
        high, low = split(vt[slot].T)
        t_high, t_low = split(t_ref[...])
        both = dot(jnp.concatenate([high, low], axis=0), t_high)
        w_high, w_low = split(both[:BLOCK] + both[BLOCK:] + dot(high, t_low))
        rows = pl.ds(slot * BLOCK, BLOCK)
        w_ref[rows, pl.ds(0, K)] = w_high
        w_ref[rows, pl.ds(K, K)] = w_low
        w_ref[rows, pl.ds(2 * K, K)] = w_high

    t_load.wait()
    for unit, step in ORDER:
        if unit == -1:
            weights(step)
            continue
        wait_step(unit, step)
        if step < len(PLANS[unit]):
            add(unit, step)
        if step < steps_of(unit) - 1:
            send(unit, step + 1)
        else:
            high, low = split(coef[unit])
            group = unit // COLORS
            columns = pl.ds((unit % COLORS * SUBS + group % SUBS) * WIDE, WIDE)
            for at, value in ((0, high), (K, high), (2 * K, low)):
                rhs[pl.ds(at + group // SUBS * HALF, HALF), columns] = value

    block = vt.at[slots[0]]
    for sem in (s1_send, s2_send, d1_send, d2_send):
        remote(block, block, sem, d1_recv, sibling).wait_send()
    rest = c_ref.at[pl.ds(0, K - K // 32), :]
    for gather in range(2):
        remote(rest, rest, out_send.at[gather], d1_recv, sibling).wait_send()


TILES = 4
TILE = ROWS // TILES


def update(c_ref, rhs, w_ref, out_hbm, obuf, sem):
    def write(tile):
        rows = pl.ds(pl.multiple_of(tile * TILE, TILE), TILE)
        return pltpu.make_async_copy(obuf.at[tile % 2], out_hbm.at[rows], sem.at[tile % 2])

    @pl.loop(0, TILES)
    def _(tile):
        @pl.when(tile >= 2)
        def _():
            write(tile - 2).wait()

        rows = pl.ds(pl.multiple_of(tile * TILE, TILE), TILE)
        obuf[tile % 2] = c_ref[rows, :] - dot(w_ref[rows, :], rhs[...])
        write(tile).start()

    write(TILES - 2).wait()
    write(TILES - 1).wait()


def shards(trailing, vectors, tfactor):
    hbm = pl.BlockSpec(memory_space=pltpu.HBM)
    vmem = pl.BlockSpec(memory_space=pltpu.VMEM)
    dma = pltpu.SemaphoreType.DMA
    cost = pl.CostEstimate(flops=2 * ROWS * COLS * K, bytes_accessed=2**24, transcendentals=0)
    c, rhs, w = pl.pallas_call(
        gather_reduce,
        out_shape=(
            pltpu.VMEM((ROWS, COLS), F32),
            pltpu.VMEM((3 * K, COLS), BF16),
            pltpu.VMEM((ROWS, 3 * K), BF16),
        ),
        in_specs=[hbm, hbm, hbm],
        out_specs=(vmem, vmem, vmem),
        scratch_shapes=[
            pltpu.VMEM((BLOCK, K), F32),
            pltpu.VMEM((K, K), F32),
            pltpu.VMEM((4, K, BLOCK), F32),
            pltpu.VMEM((PARTS, 2, PART, BLOCK // 2), F32),
            pltpu.VMEM((4, 2 * K, BLOCK), BF16),
            pltpu.VMEM((2, 2, K, BLOCK), BF16),
            pltpu.VMEM((2 * BLOCK, COLS), BF16),
            pltpu.VMEM((2 * BLOCK, COLS), BF16),
            pltpu.VMEM((UNITS, HALF, WIDE), F32),
            pltpu.VMEM((UNITS, HALF, WIDE), F32),
            pltpu.VMEM((UNITS, HALF + 24, WIDE), F32),
            dma((4,)), dma(()), dma(()),
            dma(()), dma((PARTS,)), dma(()), dma((PARTS,)),
            dma(()), dma(()), dma(()), dma((PARTS,)),
            dma((2,)), dma((UNITS, 2 * MOST)),
        ],
        compiler_params=pltpu.CompilerParams(
            collective_id=0, has_side_effects=True, vmem_limit_bytes=25 * 2**20
        ),
        cost_estimate=cost,
        name="gather_reduce",
    )(*(pltpu.with_memory_space_constraint(each, pltpu.HBM) for each in (trailing, vectors, tfactor)))
    return pl.pallas_call(
        update,
        out_shape=jax.ShapeDtypeStruct((ROWS, COLS), F32),
        in_specs=[vmem, vmem, vmem],
        out_specs=hbm,
        scratch_shapes=[pltpu.VMEM((2, TILE, COLS), F32), dma((2,))],
        compiler_params=pltpu.CompilerParams(vmem_limit_bytes=16 * 2**20),
        cost_estimate=cost,
        name="update",
    )(c, rhs, w)


def solution(mesh):
    placed = (P("row", "col"), P(("row", "col"), None), P())
    return jax.shard_map(
        shards, mesh=mesh, in_specs=placed, out_specs=P("row", "col"), check_vma=False
    )
```

```python
import jax
import jax.numpy as jnp
from jax import lax
from jax.experimental import pallas as pl
from jax.experimental.pallas import tpu as pltpu
from jax.sharding import PartitionSpec as P

MESH = pl.DeviceIdType.MESH
F32, BF16 = jnp.float32, jnp.bfloat16

ROWS = 2048
COLS = 2048
K = 256
HALF = K // 2
PARTS = 4
PART = K // PARTS
BLOCK = 512
COLORS = 4
SUBS = 2
WIDE = COLS // (COLORS * SUBS)
NEAR = 2 * WIDE
UNITS = 2 * SUBS * COLORS

PLANS = (
    (("zb",), ("xa",), ("xb", "y", "za")),
    (("xa",), ("zb",), ("xb", "y", "za")),
    (("za",), ("xb",), ("xa", "zb", "y")),
    (("xb",), ("za",), ("xa", "y", "zb")),
    (("y", "zb"), ("xa",), ("xb", "za")),
    (("xb",), ("y", "zb"), ("xa", "za")),
    (("y",), ("xb", "za"), ("xa", "zb")),
    (("zb",), ("xa",), ("xb", "y", "za")),
    (("xa",), ("y", "zb"), ("xb", "za")),
    (("y",), ("xb", "za"), ("xa", "zb")),
    (("za",), ("xa",), ("xb", "y", "zb")),
    (("xa",), ("y", "za"), ("xb", "zb")),
    (("za",), ("xa",), ("xb", "y", "zb")),
    (("xb",), ("zb",), ("xa", "za", "y")),
    (("y",), ("xb", "za"), ("xa", "zb")),
    (("zb",), ("xa",), ("xb", "y", "za")),
)
ORDER = (
    (0, 0), (1, 0), (2, 0), (3, 0), (4, 0), (5, 0), (6, 0), (7, 0),
    (8, 0), (9, 0), (10, 0), (11, 0), (12, 0), (13, 0), (14, 0), (15, 0),
    (-1, 0), (0, 1), (1, 1), (2, 1), (3, 1), (4, 1), (5, 1), (6, 1),
    (7, 1), (8, 1), (9, 1), (10, 1), (11, 1), (12, 1), (13, 1), (14, 1),
    (15, 1), (-1, 1), (0, 2), (1, 2), (2, 2), (3, 2), (4, 2), (5, 2),
    (6, 2), (7, 2), (8, 2), (9, 2), (10, 2), (11, 2), (12, 2), (13, 2),
    (14, 2), (15, 2), (-1, 2), (-1, 3), (0, 3), (1, 3), (2, 3), (3, 3),
    (4, 3), (5, 3), (6, 3), (7, 3), (8, 3), (9, 3), (10, 3), (11, 3),
    (0, 4), (1, 4), (2, 4), (3, 4), (12, 3), (13, 3), (14, 3), (15, 3),
    (4, 4), (5, 4), (6, 4), (7, 4), (8, 4), (9, 4), (10, 4), (11, 4),
    (0, 5), (1, 5), (2, 5), (3, 5), (12, 4), (13, 4), (14, 4), (15, 4),
    (8, 5), (9, 5), (10, 5), (11, 5), (-2, 0), (4, 5), (5, 5), (6, 5),
    (7, 5), (-2, 1), (12, 5), (13, 5), (14, 5), (15, 5),
)
MOST = max(len(plan) for plan in PLANS)


def split(value):
    high = value.astype(BF16)
    return high, (value - high.astype(F32)).astype(BF16)


def dot(left, right):
    return jnp.dot(left, right, preferred_element_type=F32)


def place():
    row, col = lax.axis_index("row"), lax.axis_index("col")
    z, x, y_low = row // 8, (row // 2) % 4, row % 2
    bits = {
        "xa": (x % 2 + x // 2) % 2,
        "xb": x // 2,
        "za": (z % 2 + z // 2) % 2,
        "zb": z // 2,
        "y": y_low,
    }
    return bits, col


def row_of(bits):
    x = bits["xb"] * 2 + (bits["xa"] + bits["xb"]) % 2
    z = bits["zb"] * 2 + (bits["za"] + bits["zb"]) % 2
    return z * 8 + x * 2 + bits["y"]


def flipped(bits, names):
    return {name: 1 - bit if name in names else bit for name, bit in bits.items()}


def index_of(bits, names):
    index = 0
    for name in names:
        index = index * 2 + bits[name]
    return index


def offsets(names):
    count = len(names)
    return [
        tuple(name for at, name in enumerate(names) if offset >> (count - 1 - at) & 1)
        for offset in range(1, 2**count)
    ]


def gather_reduce(
    c_hbm, v_hbm, t_hbm, c_ref, rhs, w_ref,
    v_ref, t_ref, vt, fwd, vst, vfar, c_high, c_low, part, coef, arrived, near_rhs,
    c_sem, v_sem, t_sem,
    s1_send, s1_recv, s2_send, s2_recv, d1_send, d1_recv, d2_send, d2_recv,
    out_send, out_recv,
):
    bits, col = place()
    row = row_of(bits)
    y_high, core = col // 2, col % 2
    y = y_high * 2 + bits["y"]
    sibling = (row, y_high * 2 + 1 - core)
    along = []
    for step in (1, 3):
        there = (y + step) % 4
        along.append((row - bits["y"] + there % 2, there // 2 * 2 + core))
    slots = [
        col,
        y_high * 2 + 1 - core,
        (1 - y_high) * 2 + core,
        (1 - y_high) * 2 + 1 - core,
    ]

    v_load = pltpu.make_async_copy(v_hbm, v_ref, v_sem)
    t_load = pltpu.make_async_copy(t_hbm, t_ref, t_sem)
    c_loads = []
    for at, slot in enumerate(slots):
        rows = pl.ds(pl.multiple_of(slot * BLOCK, BLOCK), BLOCK)
        c_loads.append(pltpu.make_async_copy(c_hbm.at[rows], c_ref.at[rows], c_sem.at[at]))
    v_load.start()
    c_loads[0].start()

    barrier = pltpu.get_barrier_semaphore()
    met = {frozenset(names) for plan in PLANS for stage in plan for names in offsets(stage)} | {frozenset(("y",))}
    met = sorted(sorted(names) for names in met)
    greet = [(row_of(flipped(bits, names)), col) for names in met]
    other = (y + 1) % 4 * bits["y"] + (y + 3) % 4 * (1 - bits["y"])
    greet += [sibling, (row - bits["y"] + other % 2, other // 2 * 2 + core)]
    for device in greet:
        pl.semaphore_signal(barrier, inc=1, device_id=device, device_id_type=MESH)

    v_load.wait()
    c_loads[1].start()
    t_load.start()
    vt[slots[0]] = v_ref[...].T
    pl.semaphore_wait(barrier, len(greet))

    def remote(src, dst, send, recv, device):
        return pltpu.make_async_remote_copy(
            src_ref=src, dst_ref=dst, send_sem=send, recv_sem=recv,
            device_id=device, device_id_type=MESH,
        )

    def piece(slot, q, way):
        return vt.at[slot, pl.ds(q * PART, PART), pl.ds(way * (BLOCK // 2), BLOCK // 2)]

    order = [(q, way) for q in range(PARTS) for way in range(2)]
    for q, way in order:
        remote(
            piece(slots[0], q, way), fwd.at[q, way], s1_send, s1_recv.at[q], along[way]
        ).start()
    near = remote(vt.at[slots[0]], vt.at[slots[0]], d1_send, d1_recv, sibling)
    near.start()

    def halves(slot):
        high, low = split(vt[slot])
        vst[slot, pl.ds(0, K), :] = high
        vst[slot, pl.ds(K, K), :] = low

    def unit_of(half, column):
        return half * SUBS * COLORS + column

    def whole_product(slot, fresh):
        @pl.loop(0, 2)
        def _(side):
            rows = pl.ds(pl.multiple_of(slot * BLOCK, BLOCK), BLOCK)
            columns = pl.ds(pl.multiple_of(side * 4 * WIDE, 4 * WIDE), 4 * WIDE)
            high, low = split(c_ref[rows, columns])
            both = dot(vst[slot], high)
            total = both[:K] + both[K:] + dot(vst[slot, :K], low)
            for half in range(2):
                for column in range(4):
                    unit = unit_of(half, side * 4 + column)
                    value = total[half * HALF : (half + 1) * HALF, column * WIDE : (column + 1) * WIDE]
                    if fresh:
                        part[unit] = value
                    else:
                        part[unit] += value

    halves(slots[0])
    c_loads[0].wait()
    c_loads[2].start()
    c_loads[3].start()
    whole_product(slots[0], True)
    remote(vt.at[slots[1]], vt.at[slots[1]], d1_send, d1_recv, sibling).wait_recv()
    halves(slots[1])
    c_loads[1].wait()
    whole_product(slots[1], False)

    for q in range(PARTS):
        remote(fwd.at[q], fwd.at[q], s1_send, s1_recv.at[q], along[0]).wait_recv()
        for way in range(2):
            there = (y + (1, 3)[way]) % 4
            remote(
                fwd.at[q, way], piece((1 - there // 2) * 2 + core, q, way),
                s2_send, s2_recv.at[q], along[way],
            ).start()
        if q % 2 == 0:
            c_loads[2 + q // 2].wait()

        @pl.loop(0, 4)
        def _(step):
            size = BLOCK // 8
            start = q % 2 * (BLOCK // 2) + step * size
            rows = pl.ds(pl.multiple_of(slots[2 + q // 2] * BLOCK + start, size), size)
            high, low = split(c_ref[rows, :])
            into = pl.ds(pl.multiple_of(q // 2 * BLOCK + start, size), size)
            c_high[into, :] = high
            c_low[into, :] = low

    def quarter(slot, q):
        return vt.at[slot, pl.ds(q * PART, PART)]

    def share(q):
        landed = quarter(slots[2], q)
        remote(landed, landed, s2_send, s2_recv.at[q], along[0]).wait_recv()
        remote(landed, landed, d2_send, d2_recv.at[q], sibling).start()

    def shared(q):
        landed = quarter(slots[3], q)
        remote(landed, landed, d2_send, d2_recv.at[q], sibling).wait_recv()

    def far_halves(at, half):
        high, low = split(vt[slots[2 + at], pl.ds(half * HALF, HALF), :])
        vfar[half, at, pl.ds(0, HALF), :] = high
        vfar[half, at, pl.ds(HALF, HALF), :] = low

    def far_product(at, half, start, count):
        rows, columns = pl.ds(at * BLOCK, BLOCK), pl.ds(start * WIDE, count * WIDE)
        both = dot(vfar[half, at], c_high[rows, columns])
        total = both[:HALF] + both[HALF:] + dot(
            vfar[half, at, pl.ds(0, HALF), :], c_low[rows, columns]
        )
        for column in range(count):
            part[unit_of(half, start + column)] += total[:, column * WIDE : (column + 1) * WIDE]

    bases = [[0] for _ in range(UNITS)]

    def shape_of(unit, stage):
        start, bits_so_far = 0, 0
        for names in PLANS[unit][: stage + 1]:
            last = start
            bits_so_far += len(names)
            rows = max(HALF >> bits_so_far, 8)
            start += (2 ** len(names) - 1) * rows
        return rows, WIDE if bits_so_far < 5 else WIDE // 2, last

    def shard(unit, stage, index):
        rows, columns, _ = shape_of(unit, stage)
        base = bases[unit][stage]
        if columns == WIDE:
            return pl.ds(pl.multiple_of(base + index * rows, 8), rows), pl.ds(0, WIDE)
        at = pl.ds(pl.multiple_of(index % 2 * columns, columns), columns)
        return pl.ds(pl.multiple_of(base + index // 2 * rows, 8), rows), at

    def arrival(unit, stage, at, count):
        rows, columns, start = shape_of(unit, stage)
        return arrived.at[unit, pl.ds(start + at * rows, count * rows), pl.ds(0, columns)]

    def steps_of(unit):
        return 2 * len(PLANS[unit])

    def send(unit, step):
        gather = step >= len(PLANS[unit])
        stage = steps_of(unit) - 1 - step if gather else step
        names = PLANS[unit][stage]
        for at, flip in enumerate(offsets(names)):
            there = flipped(bits, flip)
            if gather:
                src = dst = coef.at[(unit, *shard(unit, stage, index_of(bits, names)))]
            else:
                src = part.at[(unit, *shard(unit, stage, index_of(there, names)))]
                dst = arrival(unit, stage, at, 1)
            remote(
                src, dst, out_send.at[int(gather)], out_recv.at[unit, step], (row_of(there), col)
            ).start()

    def wait_step(unit, step):
        stage = min(step, steps_of(unit) - 1 - step)
        whole = arrival(unit, stage, 0, 2 ** len(PLANS[unit][stage]) - 1)
        remote(whole, whole, out_send.at[0], out_recv.at[unit, step], sibling).wait_recv()

    def add(unit, stage):
        names = PLANS[unit][stage]
        index = index_of(bits, names)
        mine = (unit, *shard(unit, stage, index))
        rows, columns, start = shape_of(unit, stage)
        total = part[mine]
        for at in range(2 ** len(names) - 1):
            total += arrived[unit, pl.ds(start + at * rows, rows), pl.ds(0, columns)]
        if stage == len(PLANS[unit]) - 1:
            coef[mine] = total
        else:
            part[mine] = total
        bases[unit].append(bases[unit][stage] + index * rows)

    share(0)
    for half in range(2):
        share(2 * half + 1)
        far_halves(0, half)
        far_product(0, half, 0, 4)
        far_product(0, half, 4, 4)
        shared(2 * half)
        shared(2 * half + 1)
        far_halves(1, half)
        for color in range(COLORS):
            far_product(1, half, color * SUBS, SUBS)
            for sub in range(SUBS):
                send(unit_of(half, color * SUBS + sub), 0)
            if half == 0 and color == 1:
                share(2)

    def weights(slot):
        high, low = split(vt[slot].T)
        t_high, t_low = split(t_ref[...])
        both = dot(jnp.concatenate([high, low], axis=0), t_high)
        w_high, w_low = split(both[:BLOCK] + both[BLOCK:] + dot(high, t_low))
        rows = pl.ds(slot * BLOCK, BLOCK)
        w_ref[rows, pl.ds(0, K)] = w_high
        w_ref[rows, pl.ds(K, K)] = w_low
        w_ref[rows, pl.ds(2 * K, K)] = w_high

    def update_piece(piece):
        rows = pl.ds(piece * (ROWS // 2), ROWS // 2)
        c_ref[rows, :NEAR] -= dot(w_ref[rows, :], near_rhs[...])

    t_load.wait()
    for unit, step in ORDER:
        if unit == -1:
            weights(step)
            continue
        if unit == -2:
            update_piece(step)
            continue
        wait_step(unit, step)
        if step < len(PLANS[unit]):
            add(unit, step)
        if step < steps_of(unit) - 1:
            send(unit, step + 1)
        else:
            high, low = split(coef[unit])
            half, column = unit // (SUBS * COLORS), unit % (SUBS * COLORS)
            into = rhs if column * WIDE >= NEAR else near_rhs
            columns = pl.ds(column * WIDE - (NEAR if into is rhs else 0), WIDE)
            for at, value in ((0, high), (K, high), (2 * K, low)):
                into[pl.ds(at + half * HALF, HALF), columns] = value

    block = vt.at[slots[0]]
    for sem in (s1_send, s2_send, d1_send, d2_send):
        remote(block, block, sem, d1_recv, sibling).wait_send()
    rest = c_ref.at[pl.ds(0, K - K // 32), :]
    for gather in range(2):
        remote(rest, rest, out_send.at[gather], d1_recv, sibling).wait_send()


TILES = 4
SLOTS = 3
TILE = ROWS // TILES


def update(c_ref, rhs, w_ref, out_hbm, obuf, near_sem, sem):
    near, far = pl.ds(0, NEAR), pl.ds(NEAR, COLS - NEAR)

    def write_near(tile):
        rows = pl.ds(pl.multiple_of(tile * TILE, TILE), TILE)
        return pltpu.make_async_copy(c_ref.at[rows, near], out_hbm.at[rows, near], near_sem.at[tile])

    def write_far(tile):
        rows = pl.ds(pl.multiple_of(tile * TILE, TILE), TILE)
        return pltpu.make_async_copy(
            obuf.at[tile % SLOTS], out_hbm.at[rows, far], sem.at[tile % SLOTS]
        )

    for tile in range(TILES):
        write_near(tile).start()

    @pl.loop(0, TILES)
    def _(tile):
        @pl.when(tile >= SLOTS)
        def _():
            write_far(tile - SLOTS).wait()

        rows = pl.ds(pl.multiple_of(tile * TILE, TILE), TILE)
        obuf[tile % SLOTS] = c_ref[rows, far] - dot(w_ref[rows, :], rhs[...])
        write_far(tile).start()

    for tile in range(TILES):
        write_near(tile).wait()
        if tile >= TILES - SLOTS:
            write_far(tile).wait()


def shards(trailing, vectors, tfactor):
    hbm = pl.BlockSpec(memory_space=pltpu.HBM)
    vmem = pl.BlockSpec(memory_space=pltpu.VMEM)
    dma = pltpu.SemaphoreType.DMA
    cost = pl.CostEstimate(flops=2 * ROWS * COLS * K, bytes_accessed=2**24, transcendentals=0)
    c, rhs, w = pl.pallas_call(
        gather_reduce,
        out_shape=(
            pltpu.VMEM((ROWS, COLS), F32),
            pltpu.VMEM((3 * K, COLS - NEAR), BF16),
            pltpu.VMEM((ROWS, 3 * K), BF16),
        ),
        in_specs=[hbm, hbm, hbm],
        out_specs=(vmem, vmem, vmem),
        scratch_shapes=[
            pltpu.VMEM((BLOCK, K), F32),
            pltpu.VMEM((K, K), F32),
            pltpu.VMEM((4, K, BLOCK), F32),
            pltpu.VMEM((PARTS, 2, PART, BLOCK // 2), F32),
            pltpu.VMEM((4, 2 * K, BLOCK), BF16),
            pltpu.VMEM((2, 2, K, BLOCK), BF16),
            pltpu.VMEM((2 * BLOCK, COLS), BF16),
            pltpu.VMEM((2 * BLOCK, COLS), BF16),
            pltpu.VMEM((UNITS, HALF, WIDE), F32),
            pltpu.VMEM((UNITS, HALF, WIDE), F32),
            pltpu.VMEM((UNITS, HALF + 24, WIDE), F32),
            pltpu.VMEM((3 * K, NEAR), BF16),
            dma((4,)), dma(()), dma(()),
            dma(()), dma((PARTS,)), dma(()), dma((PARTS,)),
            dma(()), dma(()), dma(()), dma((PARTS,)),
            dma((2,)), dma((UNITS, 2 * MOST)),
        ],
        compiler_params=pltpu.CompilerParams(
            collective_id=0, has_side_effects=True, vmem_limit_bytes=25 * 2**20
        ),
        cost_estimate=cost,
        name="gather_reduce",
    )(*(pltpu.with_memory_space_constraint(each, pltpu.HBM) for each in (trailing, vectors, tfactor)))
    return pl.pallas_call(
        update,
        out_shape=jax.ShapeDtypeStruct((ROWS, COLS), F32),
        in_specs=[vmem, vmem, vmem],
        out_specs=hbm,
        scratch_shapes=[pltpu.VMEM((SLOTS, TILE, COLS - NEAR), F32), dma((TILES,)), dma((SLOTS,))],
        compiler_params=pltpu.CompilerParams(vmem_limit_bytes=20 * 2**20),
        cost_estimate=cost,
        name="update",
    )(c, rhs, w)


def solution(mesh):
    placed = (P("row", "col"), P(("row", "col"), None), P())
    return jax.shard_map(
        shards, mesh=mesh, in_specs=placed, out_specs=P("row", "col"), check_vma=False
    )
```

```python
import jax
import jax.numpy as jnp
from jax import lax
from jax.experimental import pallas as pl
from jax.experimental.pallas import tpu as pltpu
from jax.sharding import PartitionSpec as P

MESH = pl.DeviceIdType.MESH
F32, BF16 = jnp.float32, jnp.bfloat16

ROWS = 2048
COLS = 2048
K = 256
HALF = K // 2
PARTS = 4
PART = K // PARTS
BLOCK = 512
COLORS = 4
SUBS = 2
WIDE = COLS // (COLORS * SUBS)
NEAR = 2 * WIDE
UNITS = 2 * SUBS * COLORS

PLANS = (
    (("zb",), ("xa",), ("xb", "y", "za")),
    (("xa",), ("zb",), ("xb", "y", "za")),
    (("za",), ("xb",), ("xa", "zb", "y")),
    (("xb",), ("za",), ("xa", "y", "zb")),
    (("y", "zb"), ("xa",), ("xb", "za")),
    (("xb",), ("y", "zb"), ("xa", "za")),
    (("y",), ("xb", "za"), ("xa", "zb")),
    (("zb",), ("xa",), ("xb", "y", "za")),
    (("xa",), ("y", "zb"), ("xb", "za")),
    (("y",), ("xb", "za"), ("xa", "zb")),
    (("za",), ("xa",), ("xb", "y", "zb")),
    (("xa",), ("y", "za"), ("xb", "zb")),
    (("za",), ("xa",), ("xb", "y", "zb")),
    (("xb",), ("zb",), ("xa", "za", "y")),
    (("y",), ("xb", "za"), ("xa", "zb")),
    (("zb",), ("xa",), ("xb", "y", "za")),
)
ORDER = (
    (0, 0), (1, 0), (2, 0), (3, 0), (4, 0), (5, 0), (6, 0), (7, 0),
    (8, 0), (9, 0), (10, 0), (11, 0), (12, 0), (13, 0), (14, 0), (15, 0),
    (-1, 0), (0, 1), (1, 1), (2, 1), (3, 1), (4, 1), (5, 1), (6, 1),
    (7, 1), (8, 1), (9, 1), (10, 1), (11, 1), (12, 1), (13, 1), (14, 1),
    (15, 1), (-1, 1), (0, 2), (1, 2), (2, 2), (3, 2), (4, 2), (5, 2),
    (6, 2), (7, 2), (8, 2), (9, 2), (10, 2), (11, 2), (12, 2), (13, 2),
    (14, 2), (15, 2), (-1, 2), (-1, 3), (0, 3), (1, 3), (2, 3), (3, 3),
    (4, 3), (5, 3), (6, 3), (7, 3), (8, 3), (9, 3), (10, 3), (11, 3),
    (0, 4), (1, 4), (2, 4), (3, 4), (12, 3), (13, 3), (14, 3), (15, 3),
    (4, 4), (5, 4), (6, 4), (7, 4), (8, 4), (9, 4), (10, 4), (11, 4),
    (0, 5), (1, 5), (2, 5), (3, 5), (12, 4), (13, 4), (14, 4), (15, 4),
    (8, 5), (9, 5), (10, 5), (11, 5), (-2, 0), (4, 5), (5, 5), (6, 5),
    (7, 5), (-2, 1), (12, 5), (13, 5), (14, 5), (15, 5),
)
MOST = max(len(plan) for plan in PLANS)


def split(value):
    high = value.astype(BF16)
    return high, (value - high.astype(F32)).astype(BF16)


def dot(left, right):
    return jnp.dot(left, right, preferred_element_type=F32)


def place():
    row, col = lax.axis_index("row"), lax.axis_index("col")
    z, x, y_low = row // 8, (row // 2) % 4, row % 2
    bits = {
        "xa": (x % 2 + x // 2) % 2,
        "xb": x // 2,
        "za": (z % 2 + z // 2) % 2,
        "zb": z // 2,
        "y": y_low,
    }
    return bits, col


def row_of(bits):
    x = bits["xb"] * 2 + (bits["xa"] + bits["xb"]) % 2
    z = bits["zb"] * 2 + (bits["za"] + bits["zb"]) % 2
    return z * 8 + x * 2 + bits["y"]


def flipped(bits, names):
    return {name: 1 - bit if name in names else bit for name, bit in bits.items()}


def index_of(bits, names):
    index = 0
    for name in names:
        index = index * 2 + bits[name]
    return index


def offsets(names):
    count = len(names)
    return [
        tuple(name for at, name in enumerate(names) if offset >> (count - 1 - at) & 1)
        for offset in range(1, 2**count)
    ]


def gather_reduce(
    c_hbm, v_hbm, t_hbm, c_ref, rhs, w_ref,
    v_ref, t_ref, vt, fwd, vst, vfar, c_high, c_low, part, coef, arrived, near_rhs,
    c_sem, v_sem, t_sem,
    s1_send, s1_recv, s2_send, s2_recv, d1_send, d1_recv, d2_send, d2_recv,
    out_send, out_recv,
):
    bits, col = place()
    row = row_of(bits)
    y_high, core = col // 2, col % 2
    y = y_high * 2 + bits["y"]
    sibling = (row, y_high * 2 + 1 - core)
    along = []
    for step in (1, 3):
        there = (y + step) % 4
        along.append((row - bits["y"] + there % 2, there // 2 * 2 + core))
    slots = [
        col,
        y_high * 2 + 1 - core,
        (1 - y_high) * 2 + core,
        (1 - y_high) * 2 + 1 - core,
    ]

    v_load = pltpu.make_async_copy(v_hbm, v_ref, v_sem)
    t_load = pltpu.make_async_copy(t_hbm, t_ref, t_sem)
    c_loads = []
    for at, slot in enumerate(slots):
        rows = pl.ds(pl.multiple_of(slot * BLOCK, BLOCK), BLOCK)
        c_loads.append(pltpu.make_async_copy(c_hbm.at[rows], c_ref.at[rows], c_sem.at[at]))
    v_load.start()
    c_loads[0].start()

    barrier = pltpu.get_barrier_semaphore()
    met = {frozenset(names) for plan in PLANS for stage in plan for names in offsets(stage)} | {frozenset(("y",))}
    met = sorted(sorted(names) for names in met)
    greet = [(row_of(flipped(bits, names)), col) for names in met]
    other = (y + 1) % 4 * bits["y"] + (y + 3) % 4 * (1 - bits["y"])
    greet += [sibling, (row - bits["y"] + other % 2, other // 2 * 2 + core)]
    for device in greet:
        pl.semaphore_signal(barrier, inc=1, device_id=device, device_id_type=MESH)

    v_load.wait()
    c_loads[1].start()
    t_load.start()
    vt[slots[0]] = v_ref[...].T
    pl.semaphore_wait(barrier, len(greet))

    def remote(src, dst, send, recv, device):
        return pltpu.make_async_remote_copy(
            src_ref=src, dst_ref=dst, send_sem=send, recv_sem=recv,
            device_id=device, device_id_type=MESH,
        )

    def piece(slot, q, way):
        return vt.at[slot, pl.ds(q * PART, PART), pl.ds(way * (BLOCK // 2), BLOCK // 2)]

    order = [(q, way) for q in range(PARTS) for way in range(2)]
    for q, way in order:
        remote(
            piece(slots[0], q, way), fwd.at[q, way], s1_send, s1_recv.at[q], along[way]
        ).start()
    near = remote(vt.at[slots[0]], vt.at[slots[0]], d1_send, d1_recv, sibling)
    near.start()

    def halves(slot):
        high, low = split(vt[slot])
        vst[slot, pl.ds(0, K), :] = high
        vst[slot, pl.ds(K, K), :] = low

    def unit_of(half, column):
        return half * SUBS * COLORS + column

    def whole_product(slot, fresh):
        @pl.loop(0, 2)
        def _(side):
            rows = pl.ds(pl.multiple_of(slot * BLOCK, BLOCK), BLOCK)
            columns = pl.ds(pl.multiple_of(side * 4 * WIDE, 4 * WIDE), 4 * WIDE)
            high, low = split(c_ref[rows, columns])
            both = dot(vst[slot], high)
            total = both[:K] + both[K:] + dot(vst[slot, :K], low)
            for half in range(2):
                for column in range(4):
                    unit = unit_of(half, side * 4 + column)
                    value = total[half * HALF : (half + 1) * HALF, column * WIDE : (column + 1) * WIDE]
                    if fresh:
                        part[unit] = value
                    else:
                        part[unit] += value

    halves(slots[0])
    c_loads[0].wait()
    c_loads[2].start()
    c_loads[3].start()
    whole_product(slots[0], True)
    remote(vt.at[slots[1]], vt.at[slots[1]], d1_send, d1_recv, sibling).wait_recv()
    halves(slots[1])
    c_loads[1].wait()
    whole_product(slots[1], False)

    for q in range(PARTS):
        remote(fwd.at[q], fwd.at[q], s1_send, s1_recv.at[q], along[0]).wait_recv()
        for way in range(2):
            there = (y + (1, 3)[way]) % 4
            remote(
                fwd.at[q, way], piece((1 - there // 2) * 2 + core, q, way),
                s2_send, s2_recv.at[q], along[way],
            ).start()
        if q % 2 == 0:
            c_loads[2 + q // 2].wait()

        @pl.loop(0, 4)
        def _(step):
            size = BLOCK // 8
            start = q % 2 * (BLOCK // 2) + step * size
            rows = pl.ds(pl.multiple_of(slots[2 + q // 2] * BLOCK + start, size), size)
            high, low = split(c_ref[rows, :])
            into = pl.ds(pl.multiple_of(q // 2 * BLOCK + start, size), size)
            c_high[into, :] = high
            c_low[into, :] = low

    def quarter(slot, q):
        return vt.at[slot, pl.ds(q * PART, PART)]

    def share(q):
        landed = quarter(slots[2], q)
        remote(landed, landed, s2_send, s2_recv.at[q], along[0]).wait_recv()
        remote(landed, landed, d2_send, d2_recv.at[q], sibling).start()

    def shared(q):
        landed = quarter(slots[3], q)
        remote(landed, landed, d2_send, d2_recv.at[q], sibling).wait_recv()

    def far_halves(at, half):
        high, low = split(vt[slots[2 + at], pl.ds(half * HALF, HALF), :])
        vfar[half, at, pl.ds(0, HALF), :] = high
        vfar[half, at, pl.ds(HALF, HALF), :] = low

    def far_product(at, half, start, count):
        rows, columns = pl.ds(at * BLOCK, BLOCK), pl.ds(start * WIDE, count * WIDE)
        both = dot(vfar[half, at], c_high[rows, columns])
        total = both[:HALF] + both[HALF:] + dot(
            vfar[half, at, pl.ds(0, HALF), :], c_low[rows, columns]
        )
        for column in range(count):
            part[unit_of(half, start + column)] += total[:, column * WIDE : (column + 1) * WIDE]

    bases = [[0] for _ in range(UNITS)]

    def shape_of(unit, stage):
        start, bits_so_far = 0, 0
        for names in PLANS[unit][: stage + 1]:
            last = start
            bits_so_far += len(names)
            rows = max(HALF >> bits_so_far, 8)
            start += (2 ** len(names) - 1) * rows
        return rows, WIDE if bits_so_far < 5 else WIDE // 2, last

    def shard(unit, stage, index):
        rows, columns, _ = shape_of(unit, stage)
        base = bases[unit][stage]
        if columns == WIDE:
            return pl.ds(pl.multiple_of(base + index * rows, 8), rows), pl.ds(0, WIDE)
        at = pl.ds(pl.multiple_of(index % 2 * columns, columns), columns)
        return pl.ds(pl.multiple_of(base + index // 2 * rows, 8), rows), at

    def arrival(unit, stage, at, count):
        rows, columns, start = shape_of(unit, stage)
        return arrived.at[unit, pl.ds(start + at * rows, count * rows), pl.ds(0, columns)]

    def steps_of(unit):
        return 2 * len(PLANS[unit])

    def send(unit, step):
        gather = step >= len(PLANS[unit])
        stage = steps_of(unit) - 1 - step if gather else step
        names = PLANS[unit][stage]
        for at, flip in enumerate(offsets(names)):
            there = flipped(bits, flip)
            if gather:
                src = dst = coef.at[(unit, *shard(unit, stage, index_of(bits, names)))]
            else:
                src = part.at[(unit, *shard(unit, stage, index_of(there, names)))]
                dst = arrival(unit, stage, at, 1)
            remote(
                src, dst, out_send.at[int(gather)], out_recv.at[unit, step], (row_of(there), col)
            ).start()

    def wait_step(unit, step):
        stage = min(step, steps_of(unit) - 1 - step)
        whole = arrival(unit, stage, 0, 2 ** len(PLANS[unit][stage]) - 1)
        remote(whole, whole, out_send.at[0], out_recv.at[unit, step], sibling).wait_recv()

    def add(unit, stage):
        names = PLANS[unit][stage]
        index = index_of(bits, names)
        mine = (unit, *shard(unit, stage, index))
        rows, columns, start = shape_of(unit, stage)
        total = part[mine]
        for at in range(2 ** len(names) - 1):
            total += arrived[unit, pl.ds(start + at * rows, rows), pl.ds(0, columns)]
        if stage == len(PLANS[unit]) - 1:
            coef[mine] = total
        else:
            part[mine] = total
        bases[unit].append(bases[unit][stage] + index * rows)

    share(0)
    for half in range(2):
        share(2 * half + 1)
        far_halves(0, half)
        far_product(0, half, 0, 4)
        far_product(0, half, 4, 4)
        shared(2 * half)
        shared(2 * half + 1)
        far_halves(1, half)
        for color in range(COLORS):
            far_product(1, half, color * SUBS, SUBS)
            for sub in range(SUBS):
                send(unit_of(half, color * SUBS + sub), 0)
            if half == 0 and color == 1:
                share(2)

    def weights(slot):
        high, low = split(vt[slot].T)
        t_high, t_low = split(t_ref[...])
        both = dot(jnp.concatenate([high, low], axis=0), t_high)
        w_high, w_low = split(both[:BLOCK] + both[BLOCK:] + dot(high, t_low))
        rows = pl.ds(slot * BLOCK, BLOCK)
        w_ref[rows, pl.ds(0, K)] = w_high
        w_ref[rows, pl.ds(K, K)] = w_low
        w_ref[rows, pl.ds(2 * K, K)] = w_high

    def update_piece(piece):
        rows = pl.ds(piece * (ROWS // 2), ROWS // 2)
        c_ref[rows, :NEAR] -= dot(w_ref[rows, :], near_rhs[...])

    t_load.wait()
    for unit, step in ORDER:
        if unit == -1:
            weights(step)
            continue
        if unit == -2:
            update_piece(step)
            continue
        wait_step(unit, step)
        if step < len(PLANS[unit]):
            add(unit, step)
        if step < steps_of(unit) - 1:
            send(unit, step + 1)
        else:
            high, low = split(coef[unit])
            half, column = unit // (SUBS * COLORS), unit % (SUBS * COLORS)
            into = rhs if column * WIDE >= NEAR else near_rhs
            columns = pl.ds(column * WIDE - (NEAR if into is rhs else 0), WIDE)
            for at, value in ((0, high), (K, high), (2 * K, low)):
                into[pl.ds(at + half * HALF, HALF), columns] = value

    block = vt.at[slots[0]]
    for sem in (s1_send, s2_send, d1_send, d2_send):
        remote(block, block, sem, d1_recv, sibling).wait_send()
    rest = c_ref.at[pl.ds(0, K - K // 32), :]
    for gather in range(2):
        remote(rest, rest, out_send.at[gather], d1_recv, sibling).wait_send()


TILES = ((0, 512), (512, 512), (1024, 512), (1536, 256), (1792, 256))
SLOTS = 3


def update(c_ref, rhs, w_ref, out_hbm, obuf, near_sem, sem):
    near, far = pl.ds(0, NEAR), pl.ds(NEAR, COLS - NEAR)
    near_copies, far_copies = [], []
    for at, (start, size) in enumerate(TILES):
        rows = pl.ds(start, size)
        near_copies.append(
            pltpu.make_async_copy(c_ref.at[rows, near], out_hbm.at[rows, near], near_sem.at[at])
        )
        near_copies[-1].start()
    for at, (start, size) in enumerate(TILES):
        if at >= SLOTS:
            far_copies[at - SLOTS].wait()
        rows, slot = pl.ds(start, size), at % SLOTS
        obuf[slot, :size] = c_ref[rows, far] - dot(w_ref[rows, :], rhs[...])
        far_copies.append(
            pltpu.make_async_copy(obuf.at[slot, pl.ds(0, size)], out_hbm.at[rows, far], sem.at[slot])
        )
        far_copies[-1].start()
    for copy in near_copies + far_copies[-SLOTS:]:
        copy.wait()


def shards(trailing, vectors, tfactor):
    hbm = pl.BlockSpec(memory_space=pltpu.HBM)
    vmem = pl.BlockSpec(memory_space=pltpu.VMEM)
    dma = pltpu.SemaphoreType.DMA
    cost = pl.CostEstimate(flops=2 * ROWS * COLS * K, bytes_accessed=2**24, transcendentals=0)
    c, rhs, w = pl.pallas_call(
        gather_reduce,
        out_shape=(
            pltpu.VMEM((ROWS, COLS), F32),
            pltpu.VMEM((3 * K, COLS - NEAR), BF16),
            pltpu.VMEM((ROWS, 3 * K), BF16),
        ),
        in_specs=[hbm, hbm, hbm],
        out_specs=(vmem, vmem, vmem),
        scratch_shapes=[
            pltpu.VMEM((BLOCK, K), F32),
            pltpu.VMEM((K, K), F32),
            pltpu.VMEM((4, K, BLOCK), F32),
            pltpu.VMEM((PARTS, 2, PART, BLOCK // 2), F32),
            pltpu.VMEM((4, 2 * K, BLOCK), BF16),
            pltpu.VMEM((2, 2, K, BLOCK), BF16),
            pltpu.VMEM((2 * BLOCK, COLS), BF16),
            pltpu.VMEM((2 * BLOCK, COLS), BF16),
            pltpu.VMEM((UNITS, HALF, WIDE), F32),
            pltpu.VMEM((UNITS, HALF, WIDE), F32),
            pltpu.VMEM((UNITS, HALF + 24, WIDE), F32),
            pltpu.VMEM((3 * K, NEAR), BF16),
            dma((4,)), dma(()), dma(()),
            dma(()), dma((PARTS,)), dma(()), dma((PARTS,)),
            dma(()), dma(()), dma(()), dma((PARTS,)),
            dma((2,)), dma((UNITS, 2 * MOST)),
        ],
        compiler_params=pltpu.CompilerParams(
            collective_id=0, has_side_effects=True, vmem_limit_bytes=25 * 2**20
        ),
        cost_estimate=cost,
        name="gather_reduce",
    )(*(pltpu.with_memory_space_constraint(each, pltpu.HBM) for each in (trailing, vectors, tfactor)))
    return pl.pallas_call(
        update,
        out_shape=jax.ShapeDtypeStruct((ROWS, COLS), F32),
        in_specs=[vmem, vmem, vmem],
        out_specs=hbm,
        scratch_shapes=[pltpu.VMEM((SLOTS, BLOCK, COLS - NEAR), F32), dma((len(TILES),)), dma((SLOTS,))],
        compiler_params=pltpu.CompilerParams(vmem_limit_bytes=20 * 2**20),
        cost_estimate=cost,
        name="update",
    )(c, rhs, w)


def solution(mesh):
    placed = (P("row", "col"), P(("row", "col"), None), P())
    return jax.shard_map(
        shards, mesh=mesh, in_specs=placed, out_specs=P("row", "col"), check_vma=False
    )
```
